32 devices in a mesh: cosmo: 2 (over x), row: 16 (over z, y, core).
Axes of the slice: x: 2, y: 2, z: 4, core: 2. Of those that a mesh axis runs over, the one named last changes fastest.
Arguments:
- potentials: float32 [4, 256, 16384], P('cosmo', 'row'), parts along dimension 0, may hold values from -3 to 3
- ratios: float32 [6], P('cosmo'), parts along dimension 0, may hold values from 0.3 to 0.9
- row_offset: int32 [256], P('cosmo'), parts along dimension 0, may hold values from 0 to 7
- col_offset: int32 [256], P('cosmo'), parts along dimension 0, may hold values from 0 to 127
Outputs:
- convergence: float32 [512, 16384], P(('cosmo', 'row')), parts along dimension 0
- shear_map: float32 [2, 512, 16384], P(None, ('cosmo', 'row')), parts along dimension 1
- rotation: float32 [512, 16384], P(('cosmo', 'row')), parts along dimension 0
- displacement: float32 [2, 512, 16384], P(None, ('cosmo', 'row')), parts along dimension 1
The draws below stay inside these ranges and needn't reach their ends.
There are 2 independent parts, one for each index of `cosmo`. The reference program is written for one: setup_inputs(seed, part) draws one part's arguments, and reference() takes and returns one part's arrays. A program takes and returns all parts, laid end to end along the dimension named above; each array names one. Nothing has to cross between parts.
Inputs may be any that keep to these rules, and one draw needn't show every extreme that they name: `row_offset`: row offsets count blocks of 32 rows.
All inputs are finite; a program needn't handle non-finite values.
Results may differ from the reference program's by a relative error of at most 0.00002.
Values sent between devices are 32-bit elements; how exact they have to be, the bound alone decides.
A program may use at most 128 MiB of HBM per device.

```python
import jax
import jax.numpy as jnp

NC = 16384
PLANES = 2
RB = 8
NR = 256
NCB = 128


def plant(entries, own_key, smallest, high):
    spot = [jax.random.randint(jax.random.fold_in(own_key, axis), (), 0, length) for axis, length in enumerate(entries.shape)]
    main_axis = entries.shape.index(max(entries.shape))
    neighbour = spot[:main_axis] + [(spot[main_axis] + 1) % entries.shape[main_axis]] + spot[main_axis + 1:]
    return entries.at[tuple(spot)].set(smallest).at[tuple(neighbour)].set(high)


def level_of(key, dims, split, smallest, largest):
    level = 1.0
    for position, shards_of in split:
        draws = jax.random.uniform(jax.random.fold_in(jax.random.fold_in(key, 6), position), (shards_of,), jnp.float32, smallest / len(split), largest / len(split))
        level = level * jnp.repeat(jnp.exp(draws), dims[position] // shards_of).reshape((-1,) + (1,) * (len(dims) - 1 - position))
    return level


def centred(own_key, shape, spread, reach, cuts=(), kind=jnp.bfloat16):
    values = jax.random.normal(own_key, shape, jnp.float32) * spread
    if len(cuts) > 0:
        values = level_of(own_key, shape, cuts, -0.22, 0.18) * values
    return jnp.clip(values, min=-reach, max=reach).astype(kind)


def setup_inputs(seed: int = 0, part: int = 0) -> dict:
    splits = jax.random.split(jax.random.key(seed), 5)
    part_keys = jax.random.split(jax.random.fold_in(splits[4], part), 5)
    potentials = centred(part_keys[0], (PLANES, NR, NC), 0.5, 3.0, ((1, 16),), jnp.float32)
    ratios = jnp.clip(jax.random.uniform(part_keys[1], (3,), jnp.float32, 0.3, 0.9), 0.3, 0.9)
    row_offset = plant(jax.random.randint(part_keys[2], (NCB,), 0, RB), jax.random.fold_in(part_keys[2], 1), 0, RB - 1).astype(jnp.int32)
    col_offset = plant(jax.random.randint(part_keys[3], (NCB,), 0, NCB), jax.random.fold_in(part_keys[3], 1), 0, NCB - 1).astype(jnp.int32)
    return {"potentials": potentials, "ratios": ratios, "row_offset": row_offset, "col_offset": col_offset}


def slope_along(field, direction):
    return (8.0 * (jnp.roll(field, -1, direction) - jnp.roll(field, 1, direction)) - (jnp.roll(field, -2, direction) - jnp.roll(field, 2, direction))) / 12.0


def derive_plane(potential):
    slope_r = slope_along(potential, 0)
    slope_c = slope_along(potential, 1)
    return (slope_r, slope_c, slope_along(slope_r, 0), slope_along(slope_r, 1), slope_along(slope_c, 1))


def assemble(nearer, farther, ratios):
    near_r, near_c, near_rr, near_rc, near_cc = nearer
    far_r, far_c, far_rr, far_rc, far_cc = farther
    beta_near = ratios[0]
    beta_one = ratios[1]
    beta_two = ratios[2]
    inner_rr = 1.0 - beta_near * near_rr
    inner_rc = -beta_near * near_rc
    inner_cc = 1.0 - beta_near * near_cc
    chain_rr = far_rr * inner_rr + far_rc * inner_rc
    chain_rc = far_rr * inner_rc + far_rc * inner_cc
    chain_cr = far_rc * inner_rr + far_cc * inner_rc
    chain_cc = far_rc * inner_rc + far_cc * inner_cc
    total_rr = 1.0 - beta_one * near_rr - beta_two * chain_rr
    total_rc = -beta_one * near_rc - beta_two * chain_rc
    total_cr = -beta_one * near_rc - beta_two * chain_cr
    total_cc = 1.0 - beta_one * near_cc - beta_two * chain_cc
    convergence = 1.0 - 0.5 * (total_rr + total_cc)
    shear_map = jnp.stack([0.5 * (total_rr - total_cc), -0.5 * (total_rc + total_cr)])
    rotation = 0.5 * (total_rc - total_cr)
    displacement = jnp.stack([beta_one * near_r + beta_two * far_r, beta_one * near_c + beta_two * far_c])
    return convergence, shear_map, rotation, displacement


def reference(potentials, ratios, row_offset, col_offset):
    nearer = derive_plane(potentials[0])
    derived = derive_plane(potentials[1])
    blocks = NC // 128
    source = (jnp.arange(blocks, dtype=jnp.int32) + col_offset.astype(jnp.int32)) % blocks
    lookup_rows = (jnp.arange(NR, dtype=jnp.int32)[:, None] + (NR // RB) * row_offset.astype(jnp.int32)[None, :]) % NR

    def sample(field):
        strips = field.reshape(NR, blocks, 128)
        return strips[lookup_rows, source[None, :], :].reshape(NR, NC)

    farther = tuple(sample(member) for member in derived)
    return assemble(nearer, farther, ratios)
```

```python
import functools

import jax
import jax.numpy as jnp
from jax import lax
from jax.experimental import pallas as pl
from jax.experimental.pallas import tpu as pltpu
from jax.sharding import PartitionSpec as P

RB = 8
BITS = 3
LANES = 128
HALO = 4
PER_EDGE = LANES // (2 * HALO)
FIELDS = 5
CAP = 32
LEVELS = (19, 20, 21, 22, 23, 24, 26, 28, 32)
EDGE_WINDOWS = -(-CAP // PER_EDGE)
GROUP = CAP + EDGE_WINDOWS
TILE = 16
UNROLL = 4
PASSED = (4, 3, 5, 2, 6)
DIRECT = (1, 7)
VMEM = pl.BlockSpec(memory_space=pltpu.VMEM)
ANY = pl.BlockSpec(memory_space=pl.ANY)
SMEM = pl.BlockSpec(memory_space=pltpu.SMEM)
MESH = pl.DeviceIdType.MESH


def passed_along(x, axis, by):
    size = lax.axis_size(axis)
    return lax.ppermute(x, axis, [(i, (i + by) % size) for i in range(size)])


def edge_of(left, right, lane):
    return jnp.where(lane < LANES // 2, right, left)


def columns(s, width=LANES):
    return pl.ds(pl.multiple_of(s * width, width), width)


def neighbours(b, blocks):
    return jnp.where(b == 0, blocks - 1, b - 1), jnp.where(b == blocks - 1, 0, b + 1)


def index_kernel(row_ref, col_ref, sources_ref, slot_ref, fullest_ref):
    blocks = row_ref.shape[1]
    one = jnp.bfloat16

    def dot(a, b, dims):
        return lax.dot_general(a.astype(one), b.astype(one), (dims, ((), ())), preferred_element_type=jnp.float32)

    offset = row_ref[...]
    lane = lax.broadcasted_iota(jnp.int32, (1, blocks), 1)
    source = lane + col_ref[...]
    source = jnp.where(source >= blocks, source - blocks, source)
    of_offset = (lax.broadcasted_iota(jnp.int32, (RB, blocks), 0) == offset).astype(jnp.float32)
    down = lax.broadcasted_iota(jnp.int32, (blocks, blocks), 0)
    across = lax.broadcasted_iota(jnp.int32, (blocks, blocks), 1)
    of_source = (down == source).astype(jnp.float32)
    wanted = dot(of_offset, of_source, ((1,), (1,))) > 0.5
    rank = dot(wanted.astype(jnp.float32), (down < across).astype(jnp.float32), ((1,), (0,)))
    rank = jnp.where(wanted, rank, -1.0)
    spot = lax.broadcasted_iota(jnp.int32, (CAP, blocks), 0).astype(jnp.float32)
    picks = jnp.concatenate([(rank[k : k + 1] == spot).astype(jnp.float32) for k in range(RB)], axis=0)
    names = lax.broadcasted_iota(jnp.int32, (RB, blocks), 1).astype(jnp.float32)
    sources_ref[...] = dot(names, picks, ((1,), (1,)))[:1].astype(jnp.int32)
    ranks = dot(jnp.maximum(rank, 0.0), of_source, ((1,), (0,))) * of_offset
    slot_ref[...] = jnp.sum(ranks, axis=0, keepdims=True).astype(jnp.int32) + offset * CAP
    fullest_ref[...] = jnp.broadcast_to(jnp.max(rank, keepdims=True) + 1.0, fullest_ref.shape)


def packed_group(src_ref, group, block_of, out_ref, blocks, rows):
    lane = lax.broadcasted_iota(jnp.int32, (rows, LANES), 1)
    packed = None
    for j in range(CAP):
        s = src_ref[0, group * CAP + j]
        before, after = neighbours(s, blocks)
        middle = block_of(s)
        for q in range(rows // HALO):
            out_ref[group, q, EDGE_WINDOWS + j] = middle[HALO * q : HALO * (q + 1)]
        spot = j % PER_EDGE
        edge = pltpu.roll(edge_of(block_of(before), block_of(after), lane), HALO + 2 * HALO * spot, 1)
        packed = edge if spot == 0 else jnp.where(lane >= 2 * HALO * spot, edge, packed)
        if spot == PER_EDGE - 1 or j == CAP - 1:
            for q in range(rows // HALO):
                out_ref[group, q, j // PER_EDGE] = packed[HALO * q : HALO * (q + 1)]


def pack_kernel(
    cosmos, src_ref, fullest_ref, pot_ref, out_ref, top_ref, bottom_ref, level_ref,
    near, far, levels, load_sem, level_send, level_recv,
):
    part = lax.axis_index("cosmo")
    rows, width = near.shape
    blocks = width // LANES

    def loaded(b, carry):
        pltpu.make_async_copy(pot_ref.at[1, :, columns(b)], far.at[b], load_sem.at[1]).start()
        return carry

    lax.fori_loop(0, blocks, loaded, 0, unroll=8)
    load = pltpu.make_async_copy(pot_ref.at[0], near, load_sem.at[0])
    load.start()
    peers = [{"cosmo": lax.rem(part + t, cosmos)} for t in range(1, cosmos)]
    barrier = pltpu.get_barrier_semaphore()
    for peer in peers:
        pl.semaphore_signal(barrier, inc=1, device_id=peer, device_id_type=MESH)
    pltpu.make_async_copy(far, far, load_sem.at[1]).wait()

    def group(k, carry):
        packed_group(src_ref, k, lambda s: far[s], out_ref, blocks, rows)
        return carry

    lax.fori_loop(0, RB, group, 0)
    pl.semaphore_wait(barrier, len(peers))
    copies = []
    for t, peer in enumerate(peers):
        copy = pltpu.make_async_remote_copy(
            src_ref=fullest_ref, dst_ref=levels.at[t], send_sem=level_send.at[t], recv_sem=level_recv.at[t],
            device_id=peer, device_id_type=MESH,
        )
        copy.start()
        copies.append(copy)
    load.wait()

    def rims(b, carry):
        here = columns(b)
        top_ref[:, here] = near[:HALO, here]
        bottom_ref[:, here] = near[rows - HALO :, here]
        return carry

    lax.fori_loop(0, blocks, rims, 0, unroll=8)
    for copy in copies:
        copy.wait()
    fullest = fullest_ref[...]
    for t in range(len(peers)):
        fullest = jnp.maximum(fullest, levels[t])
    tallest = jnp.max(fullest)
    level_ref[0, 0] = sum((tallest > c).astype(jnp.int32) for c in LEVELS)


def plain_pack_kernel(src_ref, pot_ref, out_ref):
    rows, width = pot_ref.shape[1:]

    def group(k, carry):
        packed_group(src_ref, k, lambda s: pot_ref[1, :, columns(s)], out_ref, width // LANES, rows)
        return carry

    lax.fori_loop(0, RB, group, 0)


def shifted(middle, edge, lane, by):
    if by > 0:
        return pltpu.roll(jnp.where(lane < by, edge, middle), LANES - by, 1)
    return pltpu.roll(jnp.where(lane >= LANES + by, edge, middle), -by, 1)


def second(x, total):
    return (
        (x[4] + x[-4]) - 16.0 * (x[3] + x[-3]) + 64.0 * (x[2] + x[-2])
        + 16.0 * (x[1] + x[-1]) - 130.0 * total
    ) * (1.0 / 144.0)


def first(x):
    return (8.0 * (x[1] - x[-1]) - (x[2] - x[-2])) * (1.0 / 12.0)


def fields(view, height):
    def middle(o):
        return view[0, HALO + o : HALO + o + height]

    def edge(o):
        return view[1, HALO + o : HALO + o + height]

    lane = lax.broadcasted_iota(jnp.int32, (height, LANES), 1)
    near = [o for o in range(-HALO, HALO + 1) if o]
    centre = middle(0)
    side = edge(0)
    along_rows = {o: middle(o) for o in near}
    slope_r = first(along_rows)
    slope_r_side = first({o: edge(o) for o in (-2, -1, 1, 2)})
    along_cols = {o: shifted(centre, side, lane, o) for o in near}
    slope_c = first(along_cols)
    curve_rc = first({o: shifted(slope_r, slope_r_side, lane, o) for o in (-2, -1, 1, 2)})
    return slope_r, slope_c, second(along_rows, centre), curve_rc, second(along_cols, centre)


def near_fields(b, view, pot, above_ref, below_ref, out_ref, here_out):
    height, width = pot.shape
    rows = height + 2 * HALO
    before, after = neighbours(b, width // LANES)
    parts = ((slice(0, HALO), above_ref), (slice(HALO, HALO + height), pot), (slice(HALO + height, rows), below_ref))
    for rim, ref in parts:
        lane = lax.broadcasted_iota(jnp.int32, (ref.shape[0], LANES), 1)
        view[0, rim] = ref[:, columns(b)]
        view[1, rim] = edge_of(ref[:, columns(before)], ref[:, columns(after)], lane)
    for n, field in enumerate(fields(view, height)):
        out_ref[n, :, here_out] = field


def far_fields(win, j, view, out_ref):
    rows = win.shape[0] * HALO
    for q in range(rows // HALO):
        view[0, HALO * q : HALO * (q + 1)] = win[q, EDGE_WINDOWS + j]
        view[1, HALO * q : HALO * (q + 1)] = win[q, lax.div(j, PER_EDGE)]
    view[1] = pltpu.roll(view[1], LANES - HALO - 2 * HALO * lax.rem(j, PER_EDGE), 1)
    for n, field in enumerate(fields(view, rows - 2 * HALO)):
        out_ref[j, n] = field


def all_far_fields(cap, win, views, out_ref):
    def some(g, carry):
        for u in range(UNROLL):
            far_fields(win, jnp.minimum(g * UNROLL + u, cap - 1), views.at[u], out_ref)
        return carry

    lax.fori_loop(0, -(-cap // UNROLL), some, 0)


def exchange_kernel(
    stride, devices, cap, buf_ref, pot_ref, top_ref, bottom_ref, near_out, far_out,
    win, pot, above, below, near, far, views, pot_sem, near_sem, far_sem, own_sem,
    send_sem, recv_sem, up_send, up_recv, down_send, down_recv,
):
    me = lax.axis_index("row")
    quads = buf_ref.shape[1]
    height, width = pot.shape
    blocks = width // LANES
    part = pl.ds(0, EDGE_WINDOWS + cap)
    load = pltpu.make_async_copy(pot_ref.at[0], pot, pot_sem)
    load.start()
    far_away = [devices - stride * k for k in range(1, RB)]
    beside = [devices - stride * k + o for k in DIRECT for o in (1, -1)]
    offsets = sorted({o % devices for o in far_away + beside + [1, -1]})
    barrier = pltpu.get_barrier_semaphore()

    def at(offset):
        return lax.rem(me + offset % devices, devices)

    for offset in offsets:
        pl.semaphore_signal(barrier, inc=1, device_id={"row": at(offset)}, device_id_type=MESH)
    pl.semaphore_wait(barrier, len(offsets))

    def sent(src, dst, send, recv, offset):
        copy = pltpu.make_async_remote_copy(
            src_ref=src, dst_ref=dst, send_sem=send, recv_sem=recv,
            device_id={"row": at(offset)}, device_id_type=MESH,
        )
        copy.start()
        return copy

    def window(k):
        return sent(
            buf_ref.at[k, :, part], win.at[k, pl.ds(1, quads), part], send_sem.at[k], recv_sem.at[k], -stride * k
        )

    def rims(k, held, low, high, offset):
        return [
            sent(held.at[k, high, part], win.at[k, 0, part], up_send.at[k], up_recv.at[k], offset + 1),
            sent(held.at[k, low, part], win.at[k, quads + 1, part], down_send.at[k], down_recv.at[k], offset - 1),
        ]

    def passed_on(k):
        return rims(k, win, 1, quads, 0)

    def straight(k):
        return rims(k, buf_ref, 0, quads - 1, -stride * k)

    windows = {PASSED[0]: window(PASSED[0])}
    near_rims = [
        sent(bottom_ref, above, up_send.at[RB], up_recv.at[RB], 1),
        sent(top_ref, below, down_send.at[RB], down_recv.at[RB], -1),
    ]
    edges = {0: straight(0)}
    for k in PASSED[1:]:
        windows[k] = window(k)
    own = pltpu.make_async_copy(buf_ref.at[0, :, part], win.at[0, pl.ds(1, quads), part], own_sem)
    own.start()
    own.wait()

    results = []

    def finish(k):
        for copy in edges[k]:
            copy.wait_recv()
        all_far_fields(cap, win.at[k], views, far.at[k])
        result = pltpu.make_async_copy(far.at[k], far_out.at[k, pl.ds(0, cap)], far_sem.at[k])
        result.start()
        results.append(result)

    finish(0)
    load.wait()
    for copy in near_rims:
        copy.wait_recv()
    wide = TILE * LANES

    def stored(c):
        here = columns(c, wide)
        return pltpu.make_async_copy(near.at[:, :, here], near_out.at[:, :, here], near_sem.at[c])

    def chunk(c, carry):
        def block(t, carry):
            b = c * TILE + t
            near_fields(b, views.at[lax.rem(t, UNROLL)], pot, above, below, near, columns(b))
            return carry

        lax.fori_loop(0, TILE, block, 0, unroll=UNROLL)
        stored(c).start()
        return carry

    lax.fori_loop(0, blocks // TILE, chunk, 0)

    direct = list(DIRECT)
    waiting = []
    for k in PASSED:
        windows[k].wait_recv()
        edges[k] = passed_on(k)
        if direct:
            extra = direct.pop(0)
            windows[extra] = window(extra)
            edges[extra] = straight(extra)
        waiting.append(k)
        if len(waiting) > 2:
            finish(waiting.pop(0))
    for k in waiting:
        finish(k)
    for k in DIRECT:
        windows[k].wait_recv()
        finish(k)
    for k in PASSED + DIRECT:
        windows[k].wait_send()
    for k in range(RB):
        for copy in edges[k]:
            copy.wait_send()
    for copy in near_rims:
        copy.wait_send()

    def drained(c, carry):
        stored(c).wait()
        return carry

    lax.fori_loop(0, blocks // TILE, drained, 0)
    for result in results:
        result.wait()


def plain_near_kernel(pot_ref, above_ref, below_ref, out_ref, view):
    step = pl.program_id(0)

    def block(t, carry):
        near_fields(step * TILE + t, view, pot_ref.at[0], above_ref, below_ref, out_ref, columns(t))
        return carry

    lax.fori_loop(0, TILE, block, 0)


def plain_far_kernel(win_ref, out_ref, view):
    def window(j, carry):
        far_fields(win_ref.at[0], j, view, out_ref.at[0])
        return carry

    lax.fori_loop(0, CAP, window, 0)


def combine_kernel(
    blocks, slot_ref, level_ref, ratio_ref, near_ref, far_hbm, conv_ref, shear_ref, rot_ref, disp_ref, far, sems,
):
    step = pl.program_id(0)
    steps = blocks // TILE
    fits = level_ref[0, 0] < len(LEVELS)
    beta_near, beta_one, beta_two = ratio_ref[0], ratio_ref[1], ratio_ref[2]

    def fetch(g):
        for t in range(TILE):
            b = g * TILE + t
            slot = jnp.where(fits, slot_ref[0, b], b)
            pltpu.make_async_copy(far_hbm.at[slot], far.at[b], sems.at[g]).start()

    @pl.when(step == 0)
    def _():
        fetch(0)
        if steps > 1:
            fetch(1)

    @pl.when(step + 2 < steps)
    def _():
        fetch(step + 2)

    mine = pl.ds(step * TILE, TILE)
    pltpu.make_async_copy(far_hbm.at[pl.ds(0, TILE)], far.at[mine], sems.at[step]).wait()

    def body(t, carry):
        there = columns(t)
        b = step * TILE + t
        near_r, near_c, near_rr, near_rc, near_cc = (near_ref[n, :, there] for n in range(FIELDS))
        far_r, far_c, far_rr, far_rc, far_cc = (far[b, n] for n in range(FIELDS))
        inner_rr = 1.0 - beta_near * near_rr
        inner_rc = -beta_near * near_rc
        inner_cc = 1.0 - beta_near * near_cc
        chain_rr = far_rr * inner_rr + far_rc * inner_rc
        chain_rc = far_rr * inner_rc + far_rc * inner_cc
        chain_cr = far_rc * inner_rr + far_cc * inner_rc
        chain_cc = far_rc * inner_rc + far_cc * inner_cc
        total_rr = 1.0 - beta_one * near_rr - beta_two * chain_rr
        total_rc = -beta_one * near_rc - beta_two * chain_rc
        total_cr = -beta_one * near_rc - beta_two * chain_cr
        total_cc = 1.0 - beta_one * near_cc - beta_two * chain_cc
        conv_ref[:, there] = 1.0 - 0.5 * (total_rr + total_cc)
        shear_ref[0, :, there] = 0.5 * (total_rr - total_cc)
        shear_ref[1, :, there] = -0.5 * (total_rc + total_cr)
        rot_ref[:, there] = 0.5 * (total_rc - total_cr)
        disp_ref[0, :, there] = beta_one * near_r + beta_two * far_r
        disp_ref[1, :, there] = beta_one * near_c + beta_two * far_c
        return carry

    lax.fori_loop(0, TILE, body, 0, unroll=4)


def per_device(potentials, ratios, row_offset, col_offset):
    devices = lax.axis_size("row")
    cosmos = lax.axis_size("cosmo")
    height, width = potentials.shape[1:]
    blocks = width // LANES
    stride = devices // RB
    quads = height // HALO
    rows = height + 2 * HALO
    wide = TILE * LANES
    f32, i32 = jnp.float32, jnp.int32
    shape = jax.ShapeDtypeStruct
    dma = pltpu.SemaphoreType.DMA

    sources, slot, fullest = pl.pallas_call(
        index_kernel,
        out_shape=(shape((1, RB * CAP), i32), shape((1, blocks), i32), shape((8, LANES), f32)),
        in_specs=[VMEM] * 2,
        out_specs=(VMEM,) * 3,
    )(row_offset.reshape(1, blocks), col_offset.reshape(1, blocks))

    packed, top, bottom, level = pl.pallas_call(
        functools.partial(pack_kernel, cosmos),
        out_shape=(
            shape((RB, quads, GROUP, HALO, LANES), f32),
            shape((HALO, width), f32),
            shape((HALO, width), f32),
            shape((1, 1), i32),
        ),
        in_specs=[SMEM, VMEM, ANY],
        out_specs=(VMEM, VMEM, VMEM, SMEM),
        scratch_shapes=[
            pltpu.VMEM((height, width), f32),
            pltpu.VMEM((blocks, height, LANES), f32),
            pltpu.VMEM((max(cosmos - 1, 1), 8, LANES), f32),
            dma((2,)),
            dma((max(cosmos - 1, 1),)),
            dma((max(cosmos - 1, 1),)),
        ],
        compiler_params=pltpu.CompilerParams(collective_id=len(LEVELS), has_side_effects=True),
    )(sources, fullest, potentials)

    near_shape = shape((FIELDS, height, width), f32)
    far_shape = shape((RB, CAP, FIELDS, height, LANES), f32)

    def direct(n, packed, potentials, top, bottom):
        cap = LEVELS[n]
        return pl.pallas_call(
            functools.partial(exchange_kernel, stride, devices, cap),
            out_shape=(near_shape, far_shape),
            in_specs=[VMEM, ANY, VMEM, VMEM],
            out_specs=(ANY, ANY),
            scratch_shapes=[
                pltpu.VMEM((RB, quads + 2, EDGE_WINDOWS + cap, HALO, LANES), f32),
                pltpu.VMEM((height, width), f32),
                pltpu.VMEM((HALO, width), f32),
                pltpu.VMEM((HALO, width), f32),
                pltpu.VMEM((FIELDS, height, width), f32),
                pltpu.VMEM((RB, cap, FIELDS, height, LANES), f32),
                pltpu.VMEM((UNROLL, 2, rows, LANES), f32),
                dma,
                dma((blocks // TILE,)),
                dma((RB,)),
                dma,
            ]
            + [dma((RB,))] * 2
            + [dma((RB + 1,))] * 4,
            compiler_params=pltpu.CompilerParams(collective_id=n, has_side_effects=True),
        )(packed, potentials, top, bottom)

    def by_bits(packed, potentials, top, bottom):
        above, below = passed_along(bottom, "row", 1), passed_along(top, "row", devices - 1)
        every = jnp.arange(RB * CAP, dtype=i32)
        source = jnp.pad((every[:blocks] + col_offset) % blocks, (0, RB * CAP - blocks))
        offsets = jnp.pad(row_offset, (0, RB * CAP - blocks)).reshape(RB, CAP)
        packed = pl.pallas_call(
            plain_pack_kernel,
            out_shape=shape((RB, quads, GROUP, HALO, LANES), f32),
            in_specs=[SMEM, VMEM],
            out_specs=VMEM,
        )(source.reshape(1, RB * CAP), potentials)
        of_edges = jnp.pad(offsets, ((0, 0), (0, EDGE_WINDOWS * PER_EDGE - CAP)))
        of_edges = jnp.repeat(of_edges.reshape(RB, EDGE_WINDOWS, PER_EDGE), 2 * HALO, axis=2)
        lanes = jnp.concatenate([of_edges, jnp.broadcast_to(offsets[:, :, None], (RB, CAP, LANES))], axis=1)
        for bit in range(BITS):
            arrived = passed_along(packed, "row", devices - stride * 2**bit)
            picked = lanes // 2**bit % 2 == 1
            packed = jnp.where(picked[:, None, :, None, :], arrived, packed)
        over = passed_along(packed[:, quads - 1 :], "row", 1)
        under = passed_along(packed[:, :1], "row", devices - 1)
        windows = jnp.concatenate([over, packed, under], axis=1)
        view = [pltpu.VMEM((2, rows, LANES), f32)]
        near = pl.pallas_call(
            plain_near_kernel,
            out_shape=near_shape,
            grid=(blocks // TILE,),
            in_specs=[pl.BlockSpec((1, height, width), lambda g: (0, 0, 0))] + [pl.BlockSpec((HALO, width), lambda g: (0, 0))] * 2,
            out_specs=pl.BlockSpec((FIELDS, height, wide), lambda g: (0, 0, g)),
            scratch_shapes=view,
        )(potentials, above, below)
        far = pl.pallas_call(
            plain_far_kernel,
            out_shape=far_shape,
            grid=(RB,),
            in_specs=[pl.BlockSpec((1, quads + 2, GROUP, HALO, LANES), lambda g: (g, 0, 0, 0, 0))],
            out_specs=pl.BlockSpec((1, CAP, FIELDS, height, LANES), lambda g: (g, 0, 0, 0, 0)),
            scratch_shapes=view,
        )(windows)
        return near, far

    branches = [functools.partial(direct, n) for n in range(len(LEVELS))] + [by_bits]
    near, far = lax.switch(level[0, 0], branches, packed, potentials, top, bottom)

    return pl.pallas_call(
        functools.partial(combine_kernel, blocks),
        out_shape=(
            shape((height, width), f32),
            shape((2, height, width), f32),
            shape((height, width), f32),
            shape((2, height, width), f32),
        ),
        grid=(blocks // TILE,),
        in_specs=[SMEM, SMEM, SMEM, pl.BlockSpec((FIELDS, height, wide), lambda g: (0, 0, g)), ANY],
        out_specs=(
            pl.BlockSpec((height, wide), lambda g: (0, g)),
            pl.BlockSpec((2, height, wide), lambda g: (0, 0, g)),
            pl.BlockSpec((height, wide), lambda g: (0, g)),
            pl.BlockSpec((2, height, wide), lambda g: (0, 0, g)),
        ),
        scratch_shapes=[pltpu.VMEM((blocks, FIELDS, height, LANES), f32), dma((blocks // TILE,))],
    )(slot, level, ratios, near, far.reshape(RB * CAP, FIELDS, height, LANES))


def solution(mesh):
    return jax.shard_map(
        per_device,
        mesh=mesh,
        in_specs=(P("cosmo", "row", None), P("cosmo"), P("cosmo"), P("cosmo")),
        out_specs=(
            P(("cosmo", "row"), None),
            P(None, ("cosmo", "row"), None),
            P(("cosmo", "row"), None),
            P(None, ("cosmo", "row"), None),
        ),
        check_vma=False,
    )
```

```python
import functools

import jax
import jax.numpy as jnp
from jax import lax
from jax.experimental import pallas as pl
from jax.experimental.pallas import tpu as pltpu
from jax.sharding import PartitionSpec as P

RB = 8
BITS = 3
LANES = 128
HALO = 4
PER_EDGE = LANES // (2 * HALO)
FIELDS = 5
CAP = 32
LEVELS = (20, 21, 22, 23, 24, 26, 32)
EDGE_WINDOWS = -(-CAP // PER_EDGE)
GROUP = CAP + EDGE_WINDOWS
TILE = 16
UNROLL = 4
ORDER = (4, 3, 5, 2, 6, 1, 7)
FIRST = 2
AHEAD = 5
LAG = 2
VMEM = pl.BlockSpec(memory_space=pltpu.VMEM)
ANY = pl.BlockSpec(memory_space=pl.ANY)
SMEM = pl.BlockSpec(memory_space=pltpu.SMEM)
MESH = pl.DeviceIdType.MESH


def passed_along(x, axis, by):
    size = lax.axis_size(axis)
    return lax.ppermute(x, axis, [(i, (i + by) % size) for i in range(size)])


def edge_of(left, right, lane):
    return jnp.where(lane < LANES // 2, right, left)


def columns(s, width=LANES):
    return pl.ds(pl.multiple_of(s * width, width), width)


def neighbours(b, blocks):
    return jnp.where(b == 0, blocks - 1, b - 1), jnp.where(b == blocks - 1, 0, b + 1)


def indices(row_ref, col_ref, sources_ref, slot_ref, fullest_ref):
    blocks = row_ref.shape[1]
    one = jnp.bfloat16

    def dot(a, b, dims):
        return lax.dot_general(a.astype(one), b.astype(one), (dims, ((), ())), preferred_element_type=jnp.float32)

    offset = row_ref[...]
    lane = lax.broadcasted_iota(jnp.int32, (1, blocks), 1)
    source = lane + col_ref[...]
    source = jnp.where(source >= blocks, source - blocks, source)
    of_offset = (lax.broadcasted_iota(jnp.int32, (RB, blocks), 0) == offset).astype(jnp.float32)
    down = lax.broadcasted_iota(jnp.int32, (blocks, blocks), 0)
    across = lax.broadcasted_iota(jnp.int32, (blocks, blocks), 1)
    of_source = (down == source).astype(jnp.float32)
    wanted = dot(of_offset, of_source, ((1,), (1,))) > 0.5
    rank = dot(wanted.astype(jnp.float32), (down < across).astype(jnp.float32), ((1,), (0,)))
    rank = jnp.where(wanted, rank, -1.0)
    spot = lax.broadcasted_iota(jnp.int32, (CAP, blocks), 0).astype(jnp.float32)
    picks = jnp.concatenate([(rank[k : k + 1] == spot).astype(jnp.float32) for k in range(RB)], axis=0)
    names = lax.broadcasted_iota(jnp.int32, (RB, blocks), 1).astype(jnp.float32)
    sources_ref[...] = dot(names, picks, ((1,), (1,)))[:1].astype(jnp.int32)
    ranks = dot(jnp.maximum(rank, 0.0), of_source, ((1,), (0,))) * of_offset
    slot_ref[...] = jnp.sum(ranks, axis=0, keepdims=True).astype(jnp.int32) + offset * CAP
    fullest_ref[...] = jnp.broadcast_to(jnp.max(rank, keepdims=True) + 1.0, fullest_ref.shape)


def packed_group(src_ref, group, block_of, out_ref, blocks, rows):
    lane = lax.broadcasted_iota(jnp.int32, (rows, LANES), 1)
    packed = None
    for j in range(CAP):
        s = src_ref[0, group * CAP + j]
        before, after = neighbours(s, blocks)
        middle = block_of(s)
        for q in range(rows // HALO):
            out_ref[group, q, EDGE_WINDOWS + j] = middle[HALO * q : HALO * (q + 1)]
        spot = j % PER_EDGE
        edge = pltpu.roll(edge_of(block_of(before), block_of(after), lane), HALO + 2 * HALO * spot, 1)
        packed = edge if spot == 0 else jnp.where(lane >= 2 * HALO * spot, edge, packed)
        if spot == PER_EDGE - 1 or j == CAP - 1:
            for q in range(rows // HALO):
                out_ref[group, q, j // PER_EDGE] = packed[HALO * q : HALO * (q + 1)]


def prepare_kernel(
    devices, cosmos, row_ref, col_ref, pot_ref, sources_ref, slot_ref, above_ref, below_ref, level_ref,
    near, top, bottom, fullest_ref, levels, load_sem, send_sem, recv_sem, level_send, level_recv,
):
    me, part = lax.axis_index("row"), lax.axis_index("cosmo")
    rows, width = near.shape
    load = pltpu.make_async_copy(pot_ref.at[0], near, load_sem)
    load.start()
    peers = [{"row": lax.rem(me + 1, devices)}, {"row": lax.rem(me + devices - 1, devices)}]
    peers += [{"cosmo": lax.rem(part + t, cosmos)} for t in range(1, cosmos)]
    barrier = pltpu.get_barrier_semaphore()
    for peer in peers:
        pl.semaphore_signal(barrier, inc=1, device_id=peer, device_id_type=MESH)
    load.wait()

    def rims(b, carry):
        here = columns(b)
        top[:, here] = near[:HALO, here]
        bottom[:, here] = near[rows - HALO :, here]
        return carry

    lax.fori_loop(0, width // LANES, rims, 0, unroll=8)
    pl.semaphore_wait(barrier, len(peers))

    def sent(src, dst, send, recv, to):
        copy = pltpu.make_async_remote_copy(
            src_ref=src, dst_ref=dst, send_sem=send, recv_sem=recv, device_id=to, device_id_type=MESH
        )
        copy.start()
        return copy

    copies = [
        sent(bottom, above_ref, send_sem.at[0], recv_sem.at[0], peers[0]),
        sent(top, below_ref, send_sem.at[1], recv_sem.at[1], peers[1]),
    ]
    indices(row_ref, col_ref, sources_ref, slot_ref, fullest_ref)
    fullest = fullest_ref[...]
    for t in range(cosmos - 1):
        copies.append(sent(fullest_ref, levels.at[t], level_send.at[t], level_recv.at[t], peers[2 + t]))
    for copy in copies:
        copy.wait()
    for t in range(cosmos - 1):
        fullest = jnp.maximum(fullest, levels[t])
    tallest = jnp.max(fullest)
    level_ref[0, 0] = sum((tallest > c).astype(jnp.int32) for c in LEVELS)


def plain_pack_kernel(src_ref, pot_ref, out_ref):
    rows, width = pot_ref.shape[1:]

    def group(k, carry):
        packed_group(src_ref, k, lambda s: pot_ref[1, :, columns(s)], out_ref, width // LANES, rows)
        return carry

    lax.fori_loop(0, RB, group, 0)


def shifted(middle, edge, lane, by):
    if by > 0:
        return pltpu.roll(jnp.where(lane < by, edge, middle), LANES - by, 1)
    return pltpu.roll(jnp.where(lane >= LANES + by, edge, middle), -by, 1)


def second(x, total):
    return (
        (x[4] + x[-4]) - 16.0 * (x[3] + x[-3]) + 64.0 * (x[2] + x[-2])
        + 16.0 * (x[1] + x[-1]) - 130.0 * total
    ) * (1.0 / 144.0)


def first(x):
    return (8.0 * (x[1] - x[-1]) - (x[2] - x[-2])) * (1.0 / 12.0)


def fields(view, height):
    def middle(o):
        return view[0, HALO + o : HALO + o + height]

    def edge(o):
        return view[1, HALO + o : HALO + o + height]

    lane = lax.broadcasted_iota(jnp.int32, (height, LANES), 1)
    near = [o for o in range(-HALO, HALO + 1) if o]
    centre = middle(0)
    side = edge(0)
    along_rows = {o: middle(o) for o in near}
    slope_r = first(along_rows)
    slope_r_side = first({o: edge(o) for o in (-2, -1, 1, 2)})
    along_cols = {o: shifted(centre, side, lane, o) for o in near}
    slope_c = first(along_cols)
    curve_rc = first({o: shifted(slope_r, slope_r_side, lane, o) for o in (-2, -1, 1, 2)})
    return slope_r, slope_c, second(along_rows, centre), curve_rc, second(along_cols, centre)


def near_fields(b, view, pot, above_ref, below_ref, out_ref, here_out):
    height, width = pot.shape
    rows = height + 2 * HALO
    before, after = neighbours(b, width // LANES)
    parts = ((slice(0, HALO), above_ref), (slice(HALO, HALO + height), pot), (slice(HALO + height, rows), below_ref))
    for rim, ref in parts:
        lane = lax.broadcasted_iota(jnp.int32, (ref.shape[0], LANES), 1)
        view[0, rim] = ref[:, columns(b)]
        view[1, rim] = edge_of(ref[:, columns(before)], ref[:, columns(after)], lane)
    for n, field in enumerate(fields(view, height)):
        out_ref[n, :, here_out] = field


def far_fields(win, j, view, out_ref):
    rows = win.shape[0] * HALO
    for q in range(rows // HALO):
        view[0, HALO * q : HALO * (q + 1)] = win[q, EDGE_WINDOWS + j]
        view[1, HALO * q : HALO * (q + 1)] = win[q, lax.div(j, PER_EDGE)]
    view[1] = pltpu.roll(view[1], LANES - HALO - 2 * HALO * lax.rem(j, PER_EDGE), 1)
    for n, field in enumerate(fields(view, rows - 2 * HALO)):
        out_ref[j, n] = field


def all_far_fields(cap, win, views, out_ref):
    def some(g, carry):
        for u in range(UNROLL):
            far_fields(win, jnp.minimum(g * UNROLL + u, cap - 1), views.at[u], out_ref)
        return carry

    lax.fori_loop(0, -(-cap // UNROLL), some, 0)


def exchange_kernel(
    stride, devices, cap, src_ref, pot_ref, above_ref, below_ref, near_out, far_out,
    plane, buf_ref, win, pot, near, far, views, plane_sem, pot_sem, near_sem, far_sem, own_sem,
    send_sem, recv_sem, up_send, up_recv, down_send, down_recv, cross_send,
):
    me = lax.axis_index("row")
    quads = buf_ref.shape[1]
    height, width = pot.shape
    blocks = width // LANES
    part = pl.ds(0, EDGE_WINDOWS + cap)

    def loaded(b, carry):
        pltpu.make_async_copy(pot_ref.at[1, :, columns(b)], plane.at[b], plane_sem).start()
        return carry

    lax.fori_loop(0, blocks, loaded, 0, unroll=8)
    load = pltpu.make_async_copy(pot_ref.at[0], pot, pot_sem)
    load.start()
    half = devices // 2
    faces_up, faces_down = lax.rem(me + 1, half) == 0, lax.rem(me, half) == 0
    feeds_up, feeds_down = lax.rem(me + 1, stride) == 0, lax.rem(me, stride) == 0
    offsets = [-stride * k for k in range(1, RB)] + [1, -1]
    barrier = pltpu.get_barrier_semaphore()

    def at(offset):
        return lax.rem(me + offset + devices, devices)

    def greet(offset):
        pl.semaphore_signal(barrier, inc=1, device_id={"row": at(offset)}, device_id_type=MESH)

    for offset in offsets:
        greet(offset)

    @pl.when(faces_down)
    def _():
        for k in range(RB):
            greet(-1 + stride * k)

    @pl.when(faces_up)
    def _():
        for k in range(RB):
            greet(1 + stride * k - devices)

    pltpu.make_async_copy(plane, plane, plane_sem).wait()

    def pack(k):
        packed_group(src_ref, k, lambda s: plane[s], buf_ref, blocks, height)

    pack(ORDER[0])
    pl.semaphore_wait(barrier, len(offsets) + jnp.where(feeds_up, 2, 0) + jnp.where(feeds_down, 2, 0))

    def remote(src, dst, send, recv, offset):
        return pltpu.make_async_remote_copy(
            src_ref=src, dst_ref=dst, send_sem=send, recv_sem=recv,
            device_id={"row": at(offset)}, device_id_type=MESH,
        )

    def window(k):
        copy = remote(
            buf_ref.at[k, :, part], win.at[k, pl.ds(1, quads), part], send_sem.at[k], recv_sem.at[k], -stride * k
        )
        copy.start()
        return copy

    def up(k, held, row, send, offset):
        return remote(held.at[k, row, part], win.at[k, 0, part], send, up_recv.at[k], offset + 1)

    def down(k, held, row, send, offset):
        return remote(held.at[k, row, part], win.at[k, quads + 1, part], send, down_recv.at[k], offset - 1)

    def straight(do):
        for n in range(2):
            @pl.when(feeds_up)
            def _():
                k = lax.rem(lax.div(me + 1, stride), RB // 2) + n * (RB // 2)
                do(up(k, buf_ref, quads - 1, cross_send.at[n], -stride * k))

            @pl.when(feeds_down)
            def _():
                k = lax.rem(lax.div(me, stride), RB // 2) + n * (RB // 2)
                do(down(k, buf_ref, 0, cross_send.at[2 + n], -stride * k))

    def passed_on(k, do):
        held, low, high = (buf_ref, 0, quads - 1) if k == 0 else (win, 1, quads)

        @pl.when(jnp.logical_not(faces_up))
        def _():
            do(up(k, held, high, up_send.at[k], 0))

        @pl.when(jnp.logical_not(faces_down))
        def _():
            do(down(k, held, low, down_send.at[k], 0))

    def start(copy):
        copy.start()

    def wait_send(copy):
        copy.wait_send()

    def edges_here(k):
        up(k, buf_ref, quads - 1, up_send.at[k], 0).wait_recv()
        down(k, buf_ref, 0, down_send.at[k], 0).wait_recv()

    windows = {}
    for i, k in enumerate(ORDER[1:] + (0,)):
        pack(k)
        if i < FIRST:
            windows[ORDER[i]] = window(ORDER[i])
    straight(start)
    passed_on(0, start)
    for k in ORDER[FIRST:AHEAD]:
        windows[k] = window(k)
    own = pltpu.make_async_copy(buf_ref.at[0, :, part], win.at[0, pl.ds(1, quads), part], own_sem)
    own.start()
    own.wait()

    results = []

    def finish(k):
        edges_here(k)
        all_far_fields(cap, win.at[k], views, far.at[k])
        result = pltpu.make_async_copy(far.at[k], far_out.at[k, pl.ds(0, cap)], far_sem.at[k])
        result.start()
        results.append(result)

    load.wait()
    wide = TILE * LANES

    def stored(c):
        here = columns(c, wide)
        return pltpu.make_async_copy(near.at[:, :, here], near_out.at[:, :, here], near_sem.at[c])

    def chunk(c, carry):
        def block(t, carry):
            b = c * TILE + t
            near_fields(b, views.at[lax.rem(t, UNROLL)], pot, above_ref, below_ref, near, columns(b))
            return carry

        lax.fori_loop(0, TILE, block, 0, unroll=UNROLL)
        stored(c).start()
        return carry

    lax.fori_loop(0, blocks // TILE, chunk, 0)
    finish(0)

    waiting = []
    for i, k in enumerate(ORDER):
        windows[k].wait_recv()
        passed_on(k, start)
        if i + AHEAD < len(ORDER):
            windows[ORDER[i + AHEAD]] = window(ORDER[i + AHEAD])
        waiting.append(k)
        if len(waiting) > LAG:
            finish(waiting.pop(0))
    for k in waiting:
        finish(k)
    for k in ORDER:
        windows[k].wait_send()
    for k in range(RB):
        passed_on(k, wait_send)
    straight(wait_send)

    def drained(c, carry):
        stored(c).wait()
        return carry

    lax.fori_loop(0, blocks // TILE, drained, 0)
    for result in results:
        result.wait()


def plain_near_kernel(pot_ref, above_ref, below_ref, out_ref, view):
    step = pl.program_id(0)

    def block(t, carry):
        near_fields(step * TILE + t, view, pot_ref.at[0], above_ref, below_ref, out_ref, columns(t))
        return carry

    lax.fori_loop(0, TILE, block, 0)


def plain_far_kernel(win_ref, out_ref, view):
    def window(j, carry):
        far_fields(win_ref.at[0], j, view, out_ref.at[0])
        return carry

    lax.fori_loop(0, CAP, window, 0)


def combine_kernel(
    blocks, slot_ref, level_ref, ratio_ref, near_ref, far_hbm, conv_ref, shear_ref, rot_ref, disp_ref, far, sems,
):
    step = pl.program_id(0)
    steps = blocks // TILE
    fits = level_ref[0, 0] < len(LEVELS)
    beta_near, beta_one, beta_two = ratio_ref[0], ratio_ref[1], ratio_ref[2]

    def fetch(g):
        for t in range(TILE):
            b = g * TILE + t
            slot = jnp.where(fits, slot_ref[0, b], b)
            pltpu.make_async_copy(far_hbm.at[slot], far.at[b], sems.at[g]).start()

    @pl.when(step == 0)
    def _():
        fetch(0)
        if steps > 1:
            fetch(1)

    @pl.when(step + 2 < steps)
    def _():
        fetch(step + 2)

    mine = pl.ds(step * TILE, TILE)
    pltpu.make_async_copy(far_hbm.at[pl.ds(0, TILE)], far.at[mine], sems.at[step]).wait()

    def body(t, carry):
        there = columns(t)
        b = step * TILE + t
        near_r, near_c, near_rr, near_rc, near_cc = (near_ref[n, :, there] for n in range(FIELDS))
        far_r, far_c, far_rr, far_rc, far_cc = (far[b, n] for n in range(FIELDS))
        inner_rr = 1.0 - beta_near * near_rr
        inner_rc = -beta_near * near_rc
        inner_cc = 1.0 - beta_near * near_cc
        chain_rr = far_rr * inner_rr + far_rc * inner_rc
        chain_rc = far_rr * inner_rc + far_rc * inner_cc
        chain_cr = far_rc * inner_rr + far_cc * inner_rc
        chain_cc = far_rc * inner_rc + far_cc * inner_cc
        total_rr = 1.0 - beta_one * near_rr - beta_two * chain_rr
        total_rc = -beta_one * near_rc - beta_two * chain_rc
        total_cr = -beta_one * near_rc - beta_two * chain_cr
        total_cc = 1.0 - beta_one * near_cc - beta_two * chain_cc
        conv_ref[:, there] = 1.0 - 0.5 * (total_rr + total_cc)
        shear_ref[0, :, there] = 0.5 * (total_rr - total_cc)
        shear_ref[1, :, there] = -0.5 * (total_rc + total_cr)
        rot_ref[:, there] = 0.5 * (total_rc - total_cr)
        disp_ref[0, :, there] = beta_one * near_r + beta_two * far_r
        disp_ref[1, :, there] = beta_one * near_c + beta_two * far_c
        return carry

    lax.fori_loop(0, TILE, body, 0, unroll=4)


def per_device(potentials, ratios, row_offset, col_offset):
    devices = lax.axis_size("row")
    cosmos = lax.axis_size("cosmo")
    height, width = potentials.shape[1:]
    blocks = width // LANES
    stride = devices // RB
    quads = height // HALO
    rows = height + 2 * HALO
    wide = TILE * LANES
    f32, i32 = jnp.float32, jnp.int32
    shape = jax.ShapeDtypeStruct
    dma = pltpu.SemaphoreType.DMA

    others = max(cosmos - 1, 1)
    sources, slot, above, below, level = pl.pallas_call(
        functools.partial(prepare_kernel, devices, cosmos),
        out_shape=(
            shape((1, RB * CAP), i32),
            shape((1, blocks), i32),
            shape((HALO, width), f32),
            shape((HALO, width), f32),
            shape((1, 1), i32),
        ),
        in_specs=[VMEM, VMEM, ANY],
        out_specs=(VMEM, VMEM, VMEM, VMEM, SMEM),
        scratch_shapes=[
            pltpu.VMEM((height, width), f32),
            pltpu.VMEM((HALO, width), f32),
            pltpu.VMEM((HALO, width), f32),
            pltpu.VMEM((8, LANES), f32),
            pltpu.VMEM((others, 8, LANES), f32),
            dma,
            dma((2,)),
            dma((2,)),
            dma((others,)),
            dma((others,)),
        ],
        compiler_params=pltpu.CompilerParams(collective_id=len(LEVELS), has_side_effects=True),
    )(row_offset.reshape(1, blocks), col_offset.reshape(1, blocks), potentials)

    near_shape = shape((FIELDS, height, width), f32)
    far_shape = shape((RB, CAP, FIELDS, height, LANES), f32)

    def direct(n, sources, potentials, above, below):
        cap = LEVELS[n]
        return pl.pallas_call(
            functools.partial(exchange_kernel, stride, devices, cap),
            out_shape=(near_shape, far_shape),
            in_specs=[SMEM, ANY, VMEM, VMEM],
            out_specs=(ANY, ANY),
            scratch_shapes=[
                pltpu.VMEM((blocks, height, LANES), f32),
                pltpu.VMEM((RB, quads, GROUP, HALO, LANES), f32),
                pltpu.VMEM((RB, quads + 2, EDGE_WINDOWS + cap, HALO, LANES), f32),
                pltpu.VMEM((height, width), f32),
                pltpu.VMEM((FIELDS, height, width), f32),
                pltpu.VMEM((RB, cap, FIELDS, height, LANES), f32),
                pltpu.VMEM((UNROLL, 2, rows, LANES), f32),
                dma,
                dma,
                dma((blocks // TILE,)),
                dma((RB,)),
                dma,
            ]
            + [dma((RB,))] * 6
            + [dma((4,))],
            compiler_params=pltpu.CompilerParams(collective_id=n, has_side_effects=True),
        )(sources, potentials, above, below)

    def by_bits(sources, potentials, above, below):
        every = jnp.arange(RB * CAP, dtype=i32)
        source = jnp.pad((every[:blocks] + col_offset) % blocks, (0, RB * CAP - blocks))
        offsets = jnp.pad(row_offset, (0, RB * CAP - blocks)).reshape(RB, CAP)
        packed = pl.pallas_call(
            plain_pack_kernel,
            out_shape=shape((RB, quads, GROUP, HALO, LANES), f32),
            in_specs=[SMEM, VMEM],
            out_specs=VMEM,
        )(source.reshape(1, RB * CAP), potentials)
        of_edges = jnp.pad(offsets, ((0, 0), (0, EDGE_WINDOWS * PER_EDGE - CAP)))
        of_edges = jnp.repeat(of_edges.reshape(RB, EDGE_WINDOWS, PER_EDGE), 2 * HALO, axis=2)
        lanes = jnp.concatenate([of_edges, jnp.broadcast_to(offsets[:, :, None], (RB, CAP, LANES))], axis=1)
        for bit in range(BITS):
            arrived = passed_along(packed, "row", devices - stride * 2**bit)
            picked = lanes // 2**bit % 2 == 1
            packed = jnp.where(picked[:, None, :, None, :], arrived, packed)
        over = passed_along(packed[:, quads - 1 :], "row", 1)
        under = passed_along(packed[:, :1], "row", devices - 1)
        windows = jnp.concatenate([over, packed, under], axis=1)
        view = [pltpu.VMEM((2, rows, LANES), f32)]
        near = pl.pallas_call(
            plain_near_kernel,
            out_shape=near_shape,
            grid=(blocks // TILE,),
            in_specs=[pl.BlockSpec((1, height, width), lambda g: (0, 0, 0))] + [pl.BlockSpec((HALO, width), lambda g: (0, 0))] * 2,
            out_specs=pl.BlockSpec((FIELDS, height, wide), lambda g: (0, 0, g)),
            scratch_shapes=view,
        )(potentials, above, below)
        far = pl.pallas_call(
            plain_far_kernel,
            out_shape=far_shape,
            grid=(RB,),
            in_specs=[pl.BlockSpec((1, quads + 2, GROUP, HALO, LANES), lambda g: (g, 0, 0, 0, 0))],
            out_specs=pl.BlockSpec((1, CAP, FIELDS, height, LANES), lambda g: (g, 0, 0, 0, 0)),
            scratch_shapes=view,
        )(windows)
        return near, far

    branches = [functools.partial(direct, n) for n in range(len(LEVELS))] + [by_bits]
    near, far = lax.switch(level[0, 0], branches, sources, potentials, above, below)

    return pl.pallas_call(
        functools.partial(combine_kernel, blocks),
        out_shape=(
            shape((height, width), f32),
            shape((2, height, width), f32),
            shape((height, width), f32),
            shape((2, height, width), f32),
        ),
        grid=(blocks // TILE,),
        in_specs=[SMEM, SMEM, SMEM, pl.BlockSpec((FIELDS, height, wide), lambda g: (0, 0, g)), ANY],
        out_specs=(
            pl.BlockSpec((height, wide), lambda g: (0, g)),
            pl.BlockSpec((2, height, wide), lambda g: (0, 0, g)),
            pl.BlockSpec((height, wide), lambda g: (0, g)),
            pl.BlockSpec((2, height, wide), lambda g: (0, 0, g)),
        ),
        scratch_shapes=[pltpu.VMEM((blocks, FIELDS, height, LANES), f32), dma((blocks // TILE,))],
    )(slot, level, ratios, near, far.reshape(RB * CAP, FIELDS, height, LANES))


def solution(mesh):
    return jax.shard_map(
        per_device,
        mesh=mesh,
        in_specs=(P("cosmo", "row", None), P("cosmo"), P("cosmo"), P("cosmo")),
        out_specs=(
            P(("cosmo", "row"), None),
            P(None, ("cosmo", "row"), None),
            P(("cosmo", "row"), None),
            P(None, ("cosmo", "row"), None),
        ),
        check_vma=False,
    )
```

```python
import functools

import jax
import jax.numpy as jnp
from jax import lax
from jax.experimental import pallas as pl
from jax.experimental.pallas import tpu as pltpu
from jax.sharding import PartitionSpec as P

RB = 8
BITS = 3
LANES = 128
HALO = 4
PER_EDGE = LANES // (2 * HALO)
FIELDS = 5
CAP = 32
LEVELS = (20, 21, 22, 23, 24, 26, 32)
EDGE_WINDOWS = -(-CAP // PER_EDGE)
GROUP = CAP + EDGE_WINDOWS
TILE = 16
SPAN = 64
UNROLL = 4
ORDER = (4, 3, 5, 2, 6, 1, 7)
FIRST = 2
AHEAD = 5
LAG = 2
PIECES = 2
VMEM = pl.BlockSpec(memory_space=pltpu.VMEM)
ANY = pl.BlockSpec(memory_space=pl.ANY)
SMEM = pl.BlockSpec(memory_space=pltpu.SMEM)
MESH = pl.DeviceIdType.MESH


def passed_along(x, axis, by):
    size = lax.axis_size(axis)
    return lax.ppermute(x, axis, [(i, (i + by) % size) for i in range(size)])


def edge_of(left, right, lane):
    return jnp.where(lane < LANES // 2, right, left)


def columns(s, width=LANES):
    return pl.ds(pl.multiple_of(s * width, width), width)


def neighbours(b, blocks):
    return jnp.where(b == 0, blocks - 1, b - 1), jnp.where(b == blocks - 1, 0, b + 1)


def indices(row_ref, col_ref, sources_ref, slot_ref, fullest_ref):
    blocks = row_ref.shape[1]
    one = jnp.bfloat16

    def dot(a, b, dims):
        return lax.dot_general(a.astype(one), b.astype(one), (dims, ((), ())), preferred_element_type=jnp.float32)

    offset = row_ref[...]
    lane = lax.broadcasted_iota(jnp.int32, (1, blocks), 1)
    source = lane + col_ref[...]
    source = jnp.where(source >= blocks, source - blocks, source)
    of_offset = (lax.broadcasted_iota(jnp.int32, (RB, blocks), 0) == offset).astype(jnp.float32)
    down = lax.broadcasted_iota(jnp.int32, (blocks, blocks), 0)
    across = lax.broadcasted_iota(jnp.int32, (blocks, blocks), 1)
    of_source = (down == source).astype(jnp.float32)
    wanted = dot(of_offset, of_source, ((1,), (1,))) > 0.5
    rank = dot(wanted.astype(jnp.float32), (down < across).astype(jnp.float32), ((1,), (0,)))
    rank = jnp.where(wanted, rank, -1.0)
    spot = lax.broadcasted_iota(jnp.int32, (CAP, blocks), 0).astype(jnp.float32)
    picks = jnp.concatenate([(rank[k : k + 1] == spot).astype(jnp.float32) for k in range(RB)], axis=0)
    names = lax.broadcasted_iota(jnp.int32, (RB, blocks), 1).astype(jnp.float32)
    sources_ref[...] = dot(names, picks, ((1,), (1,)))[:1].astype(jnp.int32)
    ranks = dot(jnp.maximum(rank, 0.0), of_source, ((1,), (0,))) * of_offset
    slot_ref[...] = jnp.sum(ranks, axis=0, keepdims=True).astype(jnp.int32) + offset * CAP
    fullest_ref[...] = jnp.broadcast_to(jnp.max(rank, keepdims=True) + 1.0, fullest_ref.shape)


def packed_group(src_ref, group, block_of, out_ref, blocks, rows):
    lane = lax.broadcasted_iota(jnp.int32, (rows, LANES), 1)
    packed = None
    for j in range(CAP):
        s = src_ref[0, group * CAP + j]
        before, after = neighbours(s, blocks)
        middle = block_of(s)
        for q in range(rows // HALO):
            out_ref[group, q, EDGE_WINDOWS + j] = middle[HALO * q : HALO * (q + 1)]
        spot = j % PER_EDGE
        edge = pltpu.roll(edge_of(block_of(before), block_of(after), lane), HALO + 2 * HALO * spot, 1)
        packed = edge if spot == 0 else jnp.where(lane >= 2 * HALO * spot, edge, packed)
        if spot == PER_EDGE - 1 or j == CAP - 1:
            for q in range(rows // HALO):
                out_ref[group, q, j // PER_EDGE] = packed[HALO * q : HALO * (q + 1)]


def prepare_kernel(
    devices, cosmos, row_ref, col_ref, pot_ref, sources_ref, slot_ref, above_ref, below_ref, level_ref,
    near, top, bottom, fullest_ref, levels, load_sem, send_sem, recv_sem, level_send, level_recv,
):
    me, part = lax.axis_index("row"), lax.axis_index("cosmo")
    rows, width = near.shape
    load = pltpu.make_async_copy(pot_ref.at[0], near, load_sem)
    load.start()
    peers = [{"row": lax.rem(me + 1, devices)}, {"row": lax.rem(me + devices - 1, devices)}]
    peers += [{"cosmo": lax.rem(part + t, cosmos)} for t in range(1, cosmos)]
    barrier = pltpu.get_barrier_semaphore()
    for peer in peers:
        pl.semaphore_signal(barrier, inc=1, device_id=peer, device_id_type=MESH)
    load.wait()

    def rims(b, carry):
        here = columns(b)
        top[:, here] = near[:HALO, here]
        bottom[:, here] = near[rows - HALO :, here]
        return carry

    lax.fori_loop(0, width // LANES, rims, 0, unroll=8)
    pl.semaphore_wait(barrier, len(peers))

    def sent(src, dst, send, recv, to):
        copy = pltpu.make_async_remote_copy(
            src_ref=src, dst_ref=dst, send_sem=send, recv_sem=recv, device_id=to, device_id_type=MESH
        )
        copy.start()
        return copy

    copies = [
        sent(bottom, above_ref, send_sem.at[0], recv_sem.at[0], peers[0]),
        sent(top, below_ref, send_sem.at[1], recv_sem.at[1], peers[1]),
    ]
    indices(row_ref, col_ref, sources_ref, slot_ref, fullest_ref)
    fullest = fullest_ref[...]
    for t in range(cosmos - 1):
        copies.append(sent(fullest_ref, levels.at[t], level_send.at[t], level_recv.at[t], peers[2 + t]))
    for copy in copies:
        copy.wait()
    for t in range(cosmos - 1):
        fullest = jnp.maximum(fullest, levels[t])
    tallest = jnp.max(fullest)
    level_ref[0, 0] = sum((tallest > c).astype(jnp.int32) for c in LEVELS)


def plain_pack_kernel(src_ref, pot_ref, out_ref):
    rows, width = pot_ref.shape[1:]

    def group(k, carry):
        packed_group(src_ref, k, lambda s: pot_ref[1, :, columns(s)], out_ref, width // LANES, rows)
        return carry

    lax.fori_loop(0, RB, group, 0)


def shifted(middle, edge, lane, by):
    if by > 0:
        return pltpu.roll(jnp.where(lane < by, edge, middle), LANES - by, 1)
    return pltpu.roll(jnp.where(lane >= LANES + by, edge, middle), -by, 1)


def second(x, total):
    return (
        (x[4] + x[-4]) - 16.0 * (x[3] + x[-3]) + 64.0 * (x[2] + x[-2])
        + 16.0 * (x[1] + x[-1]) - 130.0 * total
    ) * (1.0 / 144.0)


def first(x):
    return (8.0 * (x[1] - x[-1]) - (x[2] - x[-2])) * (1.0 / 12.0)


def fields(view, height):
    def middle(o):
        return view[0, HALO + o : HALO + o + height]

    def edge(o):
        return view[1, HALO + o : HALO + o + height]

    lane = lax.broadcasted_iota(jnp.int32, (height, LANES), 1)
    near = [o for o in range(-HALO, HALO + 1) if o]
    centre = middle(0)
    side = edge(0)
    along_rows = {o: middle(o) for o in near}
    slope_r = first(along_rows)
    slope_r_side = first({o: edge(o) for o in (-2, -1, 1, 2)})
    along_cols = {o: shifted(centre, side, lane, o) for o in near}
    slope_c = first(along_cols)
    curve_rc = first({o: shifted(slope_r, slope_r_side, lane, o) for o in (-2, -1, 1, 2)})
    return slope_r, slope_c, second(along_rows, centre), curve_rc, second(along_cols, centre)


def near_fields(b, view, pot, above_ref, below_ref, out_ref, here_out):
    height, width = pot.shape
    rows = height + 2 * HALO
    before, after = neighbours(b, width // LANES)
    parts = ((slice(0, HALO), above_ref), (slice(HALO, HALO + height), pot), (slice(HALO + height, rows), below_ref))
    for rim, ref in parts:
        lane = lax.broadcasted_iota(jnp.int32, (ref.shape[0], LANES), 1)
        view[0, rim] = ref[:, columns(b)]
        view[1, rim] = edge_of(ref[:, columns(before)], ref[:, columns(after)], lane)
    for n, field in enumerate(fields(view, height)):
        out_ref[n, :, here_out] = field


def far_fields(win, j, view, out_ref):
    rows = win.shape[0] * HALO
    for q in range(rows // HALO):
        view[0, HALO * q : HALO * (q + 1)] = win[q, EDGE_WINDOWS + j]
        view[1, HALO * q : HALO * (q + 1)] = win[q, lax.div(j, PER_EDGE)]
    view[1] = pltpu.roll(view[1], LANES - HALO - 2 * HALO * lax.rem(j, PER_EDGE), 1)
    for n, field in enumerate(fields(view, rows - 2 * HALO)):
        out_ref[j, n] = field


def all_far_fields(cap, win, views, out_ref):
    def some(g, carry):
        for u in range(UNROLL):
            far_fields(win, jnp.minimum(g * UNROLL + u, cap - 1), views.at[u], out_ref)
        return carry

    lax.fori_loop(0, -(-cap // UNROLL), some, 0)


def exchange_kernel(
    stride, devices, cap, src_ref, pot_ref, above_ref, below_ref, near_out, far_out,
    plane, buf_ref, win, pot, near, far, views, plane_sem, pot_sem, near_sem, far_sem, own_sem,
    send_sem, recv_sem, up_send, up_recv, down_send, down_recv, cross_send,
):
    me = lax.axis_index("row")
    quads = buf_ref.shape[1]
    height, width = pot.shape
    blocks = width // LANES
    part = pl.ds(0, EDGE_WINDOWS + cap)

    def loaded(b, carry):
        pltpu.make_async_copy(pot_ref.at[1, :, columns(b)], plane.at[b], plane_sem).start()
        return carry

    lax.fori_loop(0, blocks, loaded, 0, unroll=8)
    load = pltpu.make_async_copy(pot_ref.at[0], pot, pot_sem)
    load.start()
    half = devices // 2
    faces_up, faces_down = lax.rem(me + 1, half) == 0, lax.rem(me, half) == 0
    feeds_up, feeds_down = lax.rem(me + 1, stride) == 0, lax.rem(me, stride) == 0
    offsets = [-stride * k for k in range(1, RB)] + [1, -1]
    barrier = pltpu.get_barrier_semaphore()

    def at(offset):
        return lax.rem(me + offset + devices, devices)

    def greet(offset):
        pl.semaphore_signal(barrier, inc=1, device_id={"row": at(offset)}, device_id_type=MESH)

    for offset in offsets:
        greet(offset)

    @pl.when(faces_down)
    def _():
        for k in range(RB):
            greet(-1 + stride * k)

    @pl.when(faces_up)
    def _():
        for k in range(RB):
            greet(1 + stride * k - devices)

    pltpu.make_async_copy(plane, plane, plane_sem).wait()

    def pack(k):
        packed_group(src_ref, k, lambda s: plane[s], buf_ref, blocks, height)

    pack(ORDER[0])
    pl.semaphore_wait(barrier, len(offsets) + jnp.where(feeds_up, 2, 0) + jnp.where(feeds_down, 2, 0))

    def remote(src, dst, send, recv, offset):
        return pltpu.make_async_remote_copy(
            src_ref=src, dst_ref=dst, send_sem=send, recv_sem=recv,
            device_id={"row": at(offset)}, device_id_type=MESH,
        )

    def window(k):
        copy = remote(
            buf_ref.at[k, :, part], win.at[k, pl.ds(1, quads), part], send_sem.at[k], recv_sem.at[k], -stride * k
        )
        copy.start()
        return copy

    def up(k, held, row, send, offset):
        return remote(held.at[k, row, part], win.at[k, 0, part], send, up_recv.at[k], offset + 1)

    def down(k, held, row, send, offset):
        return remote(held.at[k, row, part], win.at[k, quads + 1, part], send, down_recv.at[k], offset - 1)

    def straight(do):
        for n in range(2):
            @pl.when(feeds_up)
            def _():
                k = lax.rem(lax.div(me + 1, stride), RB // 2) + n * (RB // 2)
                do(up(k, buf_ref, quads - 1, cross_send.at[n], -stride * k))

            @pl.when(feeds_down)
            def _():
                k = lax.rem(lax.div(me, stride), RB // 2) + n * (RB // 2)
                do(down(k, buf_ref, 0, cross_send.at[2 + n], -stride * k))

    def passed_on(k, do):
        held, low, high = (buf_ref, 0, quads - 1) if k == 0 else (win, 1, quads)

        @pl.when(jnp.logical_not(faces_up))
        def _():
            do(up(k, held, high, up_send.at[k], 0))

        @pl.when(jnp.logical_not(faces_down))
        def _():
            do(down(k, held, low, down_send.at[k], 0))

    def start(copy):
        copy.start()

    def wait_send(copy):
        copy.wait_send()

    def edges_here(k):
        up(k, buf_ref, quads - 1, up_send.at[k], 0).wait_recv()
        down(k, buf_ref, 0, down_send.at[k], 0).wait_recv()

    windows = {}
    for i, k in enumerate(ORDER[1:] + (0,)):
        pack(k)
        if i < FIRST:
            windows[ORDER[i]] = window(ORDER[i])
    straight(start)
    passed_on(0, start)
    for k in ORDER[FIRST:AHEAD]:
        windows[k] = window(k)
    own = pltpu.make_async_copy(buf_ref.at[0, :, part], win.at[0, pl.ds(1, quads), part], own_sem)
    own.start()
    own.wait()

    results = []

    def finish(k):
        edges_here(k)
        all_far_fields(cap, win.at[k], views, far.at[k])
        result = pltpu.make_async_copy(far.at[k], far_out.at[k, pl.ds(0, cap)], far_sem.at[k])
        result.start()
        results.append(result)

    load.wait()
    wide = TILE * LANES

    def stored(c):
        here = columns(c, wide)
        return pltpu.make_async_copy(near.at[:, :, here], near_out.at[:, :, here], near_sem.at[c])

    def chunk(c, carry):
        def block(t, carry):
            b = c * TILE + t
            near_fields(b, views.at[lax.rem(t, UNROLL)], pot, above_ref, below_ref, near, columns(b))
            return carry

        lax.fori_loop(0, TILE, block, 0, unroll=UNROLL)
        stored(c).start()
        return carry

    chunks = blocks // TILE
    pieces = [chunks * n // PIECES for n in range(PIECES + 1)]
    lax.fori_loop(0, pieces[1], chunk, 0)
    finish(0)

    waiting = []
    for i, k in enumerate(ORDER):
        windows[k].wait_recv()
        passed_on(k, start)
        if i + AHEAD < len(ORDER):
            windows[ORDER[i + AHEAD]] = window(ORDER[i + AHEAD])
        if i + 1 < PIECES:
            lax.fori_loop(pieces[i + 1], pieces[i + 2], chunk, 0)
        waiting.append(k)
        if len(waiting) > LAG:
            finish(waiting.pop(0))
    for k in waiting:
        finish(k)
    for k in ORDER:
        windows[k].wait_send()
    for k in range(RB):
        passed_on(k, wait_send)
    straight(wait_send)

    def drained(c, carry):
        stored(c).wait()
        return carry

    lax.fori_loop(0, blocks // TILE, drained, 0)
    for result in results:
        result.wait()


def plain_near_kernel(pot_ref, above_ref, below_ref, out_ref, view):
    step = pl.program_id(0)

    def block(t, carry):
        near_fields(step * TILE + t, view, pot_ref.at[0], above_ref, below_ref, out_ref, columns(t))
        return carry

    lax.fori_loop(0, TILE, block, 0)


def plain_far_kernel(win_ref, out_ref, view):
    def window(j, carry):
        far_fields(win_ref.at[0], j, view, out_ref.at[0])
        return carry

    lax.fori_loop(0, CAP, window, 0)


def combine_kernel(
    blocks, slot_ref, level_ref, ratio_ref, near_ref, far_hbm, conv_ref, shear_ref, rot_ref, disp_ref, far, sems,
):
    step = pl.program_id(0)
    steps = blocks // SPAN
    fits = level_ref[0, 0] < len(LEVELS)
    beta_near, beta_one, beta_two = ratio_ref[0], ratio_ref[1], ratio_ref[2]

    def fetch(g):
        for t in range(SPAN):
            b = g * SPAN + t
            slot = jnp.where(fits, slot_ref[0, b], b)
            pltpu.make_async_copy(far_hbm.at[slot], far.at[b], sems.at[g]).start()

    @pl.when(step == 0)
    def _():
        fetch(0)
        if steps > 1:
            fetch(1)

    @pl.when(step + 2 < steps)
    def _():
        fetch(step + 2)

    mine = pl.ds(step * SPAN, SPAN)
    pltpu.make_async_copy(far_hbm.at[pl.ds(0, SPAN)], far.at[mine], sems.at[step]).wait()

    def body(t, carry):
        there = columns(t)
        b = step * SPAN + t
        near_r, near_c, near_rr, near_rc, near_cc = (near_ref[n, :, there] for n in range(FIELDS))
        far_r, far_c, far_rr, far_rc, far_cc = (far[b, n] for n in range(FIELDS))
        inner_rr = 1.0 - beta_near * near_rr
        inner_rc = -beta_near * near_rc
        inner_cc = 1.0 - beta_near * near_cc
        chain_rr = far_rr * inner_rr + far_rc * inner_rc
        chain_rc = far_rr * inner_rc + far_rc * inner_cc
        chain_cr = far_rc * inner_rr + far_cc * inner_rc
        chain_cc = far_rc * inner_rc + far_cc * inner_cc
        total_rr = 1.0 - beta_one * near_rr - beta_two * chain_rr
        total_rc = -beta_one * near_rc - beta_two * chain_rc
        total_cr = -beta_one * near_rc - beta_two * chain_cr
        total_cc = 1.0 - beta_one * near_cc - beta_two * chain_cc
        conv_ref[:, there] = 1.0 - 0.5 * (total_rr + total_cc)
        shear_ref[0, :, there] = 0.5 * (total_rr - total_cc)
        shear_ref[1, :, there] = -0.5 * (total_rc + total_cr)
        rot_ref[:, there] = 0.5 * (total_rc - total_cr)
        disp_ref[0, :, there] = beta_one * near_r + beta_two * far_r
        disp_ref[1, :, there] = beta_one * near_c + beta_two * far_c
        return carry

    lax.fori_loop(0, SPAN, body, 0, unroll=4)


def per_device(potentials, ratios, row_offset, col_offset):
    devices = lax.axis_size("row")
    cosmos = lax.axis_size("cosmo")
    height, width = potentials.shape[1:]
    blocks = width // LANES
    stride = devices // RB
    quads = height // HALO
    rows = height + 2 * HALO
    wide, span = TILE * LANES, SPAN * LANES
    f32, i32 = jnp.float32, jnp.int32
    shape = jax.ShapeDtypeStruct
    dma = pltpu.SemaphoreType.DMA

    others = max(cosmos - 1, 1)
    sources, slot, above, below, level = pl.pallas_call(
        functools.partial(prepare_kernel, devices, cosmos),
        out_shape=(
            shape((1, RB * CAP), i32),
            shape((1, blocks), i32),
            shape((HALO, width), f32),
            shape((HALO, width), f32),
            shape((1, 1), i32),
        ),
        in_specs=[VMEM, VMEM, ANY],
        out_specs=(VMEM, VMEM, VMEM, VMEM, SMEM),
        scratch_shapes=[
            pltpu.VMEM((height, width), f32),
            pltpu.VMEM((HALO, width), f32),
            pltpu.VMEM((HALO, width), f32),
            pltpu.VMEM((8, LANES), f32),
            pltpu.VMEM((others, 8, LANES), f32),
            dma,
            dma((2,)),
            dma((2,)),
            dma((others,)),
            dma((others,)),
        ],
        compiler_params=pltpu.CompilerParams(collective_id=len(LEVELS), has_side_effects=True),
    )(row_offset.reshape(1, blocks), col_offset.reshape(1, blocks), potentials)

    near_shape = shape((FIELDS, height, width), f32)
    far_shape = shape((RB, CAP, FIELDS, height, LANES), f32)

    def direct(n, sources, potentials, above, below):
        cap = LEVELS[n]
        return pl.pallas_call(
            functools.partial(exchange_kernel, stride, devices, cap),
            out_shape=(near_shape, far_shape),
            in_specs=[SMEM, ANY, VMEM, VMEM],
            out_specs=(ANY, ANY),
            scratch_shapes=[
                pltpu.VMEM((blocks, height, LANES), f32),
                pltpu.VMEM((RB, quads, GROUP, HALO, LANES), f32),
                pltpu.VMEM((RB, quads + 2, EDGE_WINDOWS + cap, HALO, LANES), f32),
                pltpu.VMEM((height, width), f32),
                pltpu.VMEM((FIELDS, height, width), f32),
                pltpu.VMEM((RB, cap, FIELDS, height, LANES), f32),
                pltpu.VMEM((UNROLL, 2, rows, LANES), f32),
                dma,
                dma,
                dma((blocks // TILE,)),
                dma((RB,)),
                dma,
            ]
            + [dma((RB,))] * 6
            + [dma((4,))],
            compiler_params=pltpu.CompilerParams(collective_id=n, has_side_effects=True),
        )(sources, potentials, above, below)

    def by_bits(sources, potentials, above, below):
        every = jnp.arange(RB * CAP, dtype=i32)
        source = jnp.pad((every[:blocks] + col_offset) % blocks, (0, RB * CAP - blocks))
        offsets = jnp.pad(row_offset, (0, RB * CAP - blocks)).reshape(RB, CAP)
        packed = pl.pallas_call(
            plain_pack_kernel,
            out_shape=shape((RB, quads, GROUP, HALO, LANES), f32),
            in_specs=[SMEM, VMEM],
            out_specs=VMEM,
        )(source.reshape(1, RB * CAP), potentials)
        of_edges = jnp.pad(offsets, ((0, 0), (0, EDGE_WINDOWS * PER_EDGE - CAP)))
        of_edges = jnp.repeat(of_edges.reshape(RB, EDGE_WINDOWS, PER_EDGE), 2 * HALO, axis=2)
        lanes = jnp.concatenate([of_edges, jnp.broadcast_to(offsets[:, :, None], (RB, CAP, LANES))], axis=1)
        for bit in range(BITS):
            arrived = passed_along(packed, "row", devices - stride * 2**bit)
            picked = lanes // 2**bit % 2 == 1
            packed = jnp.where(picked[:, None, :, None, :], arrived, packed)
        over = passed_along(packed[:, quads - 1 :], "row", 1)
        under = passed_along(packed[:, :1], "row", devices - 1)
        windows = jnp.concatenate([over, packed, under], axis=1)
        view = [pltpu.VMEM((2, rows, LANES), f32)]
        near = pl.pallas_call(
            plain_near_kernel,
            out_shape=near_shape,
            grid=(blocks // TILE,),
            in_specs=[pl.BlockSpec((1, height, width), lambda g: (0, 0, 0))] + [pl.BlockSpec((HALO, width), lambda g: (0, 0))] * 2,
            out_specs=pl.BlockSpec((FIELDS, height, wide), lambda g: (0, 0, g)),
            scratch_shapes=view,
        )(potentials, above, below)
        far = pl.pallas_call(
            plain_far_kernel,
            out_shape=far_shape,
            grid=(RB,),
            in_specs=[pl.BlockSpec((1, quads + 2, GROUP, HALO, LANES), lambda g: (g, 0, 0, 0, 0))],
            out_specs=pl.BlockSpec((1, CAP, FIELDS, height, LANES), lambda g: (g, 0, 0, 0, 0)),
            scratch_shapes=view,
        )(windows)
        return near, far

    branches = [functools.partial(direct, n) for n in range(len(LEVELS))] + [by_bits]
    near, far = lax.switch(level[0, 0], branches, sources, potentials, above, below)

    return pl.pallas_call(
        functools.partial(combine_kernel, blocks),
        out_shape=(
            shape((height, width), f32),
            shape((2, height, width), f32),
            shape((height, width), f32),
            shape((2, height, width), f32),
        ),
        grid=(blocks // SPAN,),
        in_specs=[SMEM, SMEM, SMEM, pl.BlockSpec((FIELDS, height, span), lambda g: (0, 0, g)), ANY],
        out_specs=(
            pl.BlockSpec((height, span), lambda g: (0, g)),
            pl.BlockSpec((2, height, span), lambda g: (0, 0, g)),
            pl.BlockSpec((height, span), lambda g: (0, g)),
            pl.BlockSpec((2, height, span), lambda g: (0, 0, g)),
        ),
        scratch_shapes=[pltpu.VMEM((blocks, FIELDS, height, LANES), f32), dma((blocks // SPAN,))],
    )(slot, level, ratios, near, far.reshape(RB * CAP, FIELDS, height, LANES))


def solution(mesh):
    return jax.shard_map(
        per_device,
        mesh=mesh,
        in_specs=(P("cosmo", "row", None), P("cosmo"), P("cosmo"), P("cosmo")),
        out_specs=(
            P(("cosmo", "row"), None),
            P(None, ("cosmo", "row"), None),
            P(("cosmo", "row"), None),
            P(None, ("cosmo", "row"), None),
        ),
        check_vma=False,
    )
```
